256 devices in a mesh: replica: 2 (over z), expert: 64 (over y, x), sub: 2 (over core).
Axes of the slice: x: 8, y: 8, z: 2, core: 2. Of those that a mesh axis runs over, the one named last changes fastest.
The devices are a block of a 8x8x16 slice.
Arguments:
- tokens: bfloat16 [2048, 7168], P(('replica', 'expert', 'sub')), parts along dimension 0, may hold values from -6 to 6
- expert_ids: int32 [2048, 8], P(('replica', 'expert', 'sub')), parts along dimension 0, may hold values from 0 to 31, all different within a row; in each aligned block of 8 rows (0 to 7, 8 to 15, ...) at most 3 rows name the same one
- route_levels: int32 [2048, 8], P(('replica', 'expert', 'sub')), parts along dimension 0, may hold values from 1 to 255
- gate_proj: bfloat16 [64, 7168, 512], P('expert', None, 'sub'), may hold values from -0.0625 to 0.0625
- up_proj: bfloat16 [64, 7168, 512], P('expert', None, 'sub'), may hold values from -0.0625 to 0.0625
- down_proj: bfloat16 [64, 512, 7168], P('expert', 'sub'), may hold values from -0.1875 to 0.1875
Outputs:
- moe_out: bfloat16 [2048, 7168], P(('replica', 'expert', 'sub')), parts along dimension 0
The draws below stay inside these ranges and needn't reach their ends.
There are 2 independent parts, one for each index of `replica`. The reference program is written for one: setup_inputs(seed, part) draws one part's arguments, and reference() takes and returns one part's arrays. A program takes and returns all parts, laid end to end along the dimension named above; an argument that names none is the same for every part. Nothing has to cross between parts.
Inputs may be any that keep to these rules, and one draw needn't show every extreme that they name: `expert_ids`: each row names 8 different experts; among the 8 rows of one device no expert is named more than 3 times, and in some devices' rows one is named exactly 3 times.
All inputs are finite; a program needn't handle non-finite values.
Results may differ from the reference program's by a relative error of at most 0.013.
Values may be sent and summed in bfloat16 or wider, within the bound.
A program may use at most 448 MiB of HBM per device.

```python
import math
import jax
import jax.numpy as jnp
import numpy as np
from jax import lax

D = 7168
FF = 1024
TOK_DEV = 8
EXPERTS = 32
TOPK = 8
CAP = 3
TOKENS = 1024
N_EXPERT = 64
N_SUB = 2


def set_ends(array, rng, least, top_value):
    shape = array.shape
    spot = [jax.random.randint(jax.random.fold_in(rng, axis), (), 0, shape[axis]) for axis in range(len(shape))]
    array = array.at[tuple(spot)].set(least)
    longest = shape.index(max(shape))
    spot[longest] = (spot[longest] + 1) % shape[longest]
    return array.at[tuple(spot)].set(top_value)


def block_levels(own_key, shape, cuts, smallest, largest):
    level, own = 1.0, jax.random.fold_in(own_key, 6)
    for dim, parts in cuts:
        draws = jnp.exp(jax.random.uniform(jax.random.fold_in(own, dim), (parts,), jnp.float32, smallest / len(cuts), largest / len(cuts)))
        level = level * jnp.repeat(draws, shape[dim] // parts).reshape([-1 if axis == dim else 1 for axis in range(len(shape))])
    return level


def deal_out(key, own, number, rows, amount, top, bound, lean):
    ranking = jax.random.permutation(key, amount)
    heavy_load, common = portions_of(amount, rows * top, bound, lean, True), portions_of(amount, rows * top, bound, lean, False)
    places = jnp.arange(amount)

    def named(lengths, offset_by):
        used = int((lengths > 0).sum())
        fixed = max(1, used // 4)
        passed = fixed + (places - fixed + offset_by * (used - fixed)) % max(1, amount - fixed)
        return jnp.zeros((amount,), jnp.int32).at[ranking[jnp.where(places < fixed, places, passed)]].set(jnp.asarray(lengths, jnp.int32))

    lengths = jnp.where(number % 4 == 0, named(heavy_load, number // 4), named(common, number - number // 4 - 1))
    mixed = jax.random.permutation(jax.random.fold_in(own, 3), amount)
    giver, taker = mixed[0:amount // 2 * 2:2], mixed[1:amount // 2 * 2:2]
    room = jnp.minimum(lengths[giver] - 1, bound - lengths[taker]) // 2
    room = jnp.where((giver == ranking[0]) | (taker == ranking[0]) | (lengths[taker] == 0), 0, jnp.maximum(room, 0))
    passed = jax.random.randint(jax.random.fold_in(own, 4), (amount // 2,), 0, 1 << 20) % (room + 1)
    lengths = lengths.at[giver].add(-passed).at[taker].add(passed)
    labels = jnp.searchsorted(jnp.cumsum(lengths), jnp.arange(rows * top), side="right").astype(jnp.int32)
    grid = labels.reshape(top, rows).T
    grid = grid[jax.random.permutation(jax.random.fold_in(own, 1), rows)]
    offset_by = jax.random.randint(jax.random.fold_in(own, 2), (rows, 1), 0, top)
    return jnp.take_along_axis(grid, (jnp.arange(top)[None, :] + offset_by) % top, axis=1)


def portions_of(count, total, bound, slope, full):
    portions = [(1 << 20) // math.isqrt(grade ** slope) + 1 for grade in range(1, count + 1)]
    largest = bound if full else min(bound, max(-(-total // count), total * portions[0] // sum(portions)))
    least = 1 if total - largest >= count - 1 else 0
    holding, surplus = [largest] + [least] * (count - 1), total - largest - least * (count - 1)
    while surplus > 0:
        free = [i for i in range(1, count) if holding[i] < largest] or [i for i in range(1, count) if holding[i] < bound]
        mass, budget = sum([portions[i] for i in free]), surplus
        for i in free:
            addition = min(bound - holding[i], max(1, budget * portions[i] // mass), surplus)
            holding[i] = holding[i] + addition
            surplus = surplus - addition
    return np.array(holding)


def noise(rng, dims, scale, most, split=(), held_as=jnp.bfloat16):
    drawn = jax.random.normal(rng, dims, jnp.float32) * scale
    if len(split) > 0:
        drawn = block_levels(rng, dims, split, -0.22, 0.18) * drawn
    return jnp.clip(drawn, min=-most, max=most).astype(held_as)


def setup_inputs(seed: int = 0, part: int = 0) -> dict:
    splits = jax.random.split(jax.random.key(seed), 7)
    own_keys = jax.random.split(jax.random.fold_in(splits[6], part), 7)
    tokens = noise(own_keys[0], (TOKENS, D), 1.0, 6.0, ((0, 128),))
    expert_ids_keys = jax.random.split(jax.random.fold_in(own_keys[1], 1), TOKENS // TOK_DEV)
    expert_ids_turns = jax.random.permutation(jax.random.fold_in(own_keys[1], 3), TOKENS // TOK_DEV)
    expert_ids = jax.vmap(lambda own, number: deal_out(jax.random.fold_in(own_keys[1], 2), own, number, TOK_DEV, EXPERTS, TOPK, CAP, 2))(expert_ids_keys, expert_ids_turns).reshape((TOKENS, TOPK))
    route_levels = set_ends(jax.random.randint(own_keys[2], (TOKENS, TOPK), 1, 256), jax.random.fold_in(own_keys[2], 1), 1, 255).astype(jnp.int32)
    gate_proj = noise(splits[3], (2 * EXPERTS, D, FF // 2), D ** -0.5, 0.0625, ((0, 64), (2, 2)))
    up_proj = noise(splits[4], (2 * EXPERTS, D, FF // 2), D ** -0.5, 0.0625, ((0, 64), (2, 2)))
    down_proj = noise(splits[5], (2 * EXPERTS, FF // 2, D), FF ** -0.5, 0.1875, ((0, 64), (1, 2)))
    return {"tokens": tokens, "expert_ids": expert_ids, "route_levels": route_levels, "gate_proj": gate_proj, "up_proj": up_proj, "down_proj": down_proj}


def reference(tokens, expert_ids, route_levels, gate_proj, up_proj, down_proj):
    devices = N_EXPERT * N_SUB
    quarter = FF // 4
    source = tokens.reshape(devices, TOK_DEV, D).astype(jnp.float32)
    picked = expert_ids.reshape(devices, TOK_DEV * TOPK)
    onehot = (picked[:, :, None] == jnp.arange(EXPERTS, dtype=jnp.int32)[None, None, :]).astype(jnp.int32)
    before = jnp.cumsum(onehot, axis=1, dtype=jnp.int32) - onehot
    slot_of = jnp.sum(before * onehot, axis=2)
    shares = route_levels.astype(jnp.float32)
    shares = shares / jnp.sum(shares, axis=1, keepdims=True)
    shares = shares.reshape(devices, TOK_DEV, TOPK)
    slot_range = jnp.arange(CAP, dtype=jnp.int32)

    def advance(running, expert):
        chosen = (picked == expert)[:, :, None] & (slot_of[:, :, None] == slot_range[None, None, :])
        placed = chosen.astype(jnp.float32).reshape(devices, TOK_DEV, TOPK, CAP)
        sender = jnp.sum(placed, axis=2)
        weighting = jnp.sum(placed * shares[:, :, :, None], axis=2)
        slot_rows = jnp.einsum("dtc,dtf->dcf", sender, source).astype(jnp.bfloat16).reshape(devices * CAP, D)
        index_low = (2 * expert).astype(jnp.int32)
        index_high = (2 * expert + 1).astype(jnp.int32)
        gate_full = jnp.concatenate([lax.dynamic_index_in_dim(gate_proj, index_low, 0, keepdims=False),
                                     lax.dynamic_index_in_dim(gate_proj, index_high, 0, keepdims=False)], axis=1)
        up_full = jnp.concatenate([lax.dynamic_index_in_dim(up_proj, index_low, 0, keepdims=False),
                                   lax.dynamic_index_in_dim(up_proj, index_high, 0, keepdims=False)], axis=1)
        down_full = jnp.concatenate([lax.dynamic_index_in_dim(down_proj, index_low, 0, keepdims=False),
                                     lax.dynamic_index_in_dim(down_proj, index_high, 0, keepdims=False)], axis=0)
        gate_vals = jnp.dot(slot_rows, gate_full, preferred_element_type=jnp.float32)
        up_vals = jnp.dot(slot_rows, up_full, preferred_element_type=jnp.float32)
        hidden = (jax.nn.silu(gate_vals) * up_vals).astype(jnp.bfloat16)
        summed = jnp.zeros((devices * CAP, D), jnp.float32)
        for portion in range(4):
            piece = jnp.dot(hidden[:, portion * quarter:(portion + 1) * quarter],
                            down_full[portion * quarter:(portion + 1) * quarter],
                            preferred_element_type=jnp.float32).astype(jnp.bfloat16)
            piece = lax.optimization_barrier(piece)
            summed = summed + piece.astype(jnp.float32)
        rounded = lax.optimization_barrier(summed.astype(jnp.bfloat16))
        expert_out = rounded.astype(jnp.float32).reshape(devices, CAP, D)
        running = running + jnp.einsum("dtc,dcf->dtf", weighting, expert_out, precision=lax.Precision.HIGHEST)
        return running, None

    start = jnp.zeros((devices, TOK_DEV, D), jnp.float32)
    running, _ = lax.scan(advance, start, jnp.arange(EXPERTS, dtype=jnp.int32))
    return running.reshape(devices * TOK_DEV, D).astype(jnp.bfloat16)
```

```python
import jax
import jax.numpy as jnp
from jax import lax
from jax.sharding import PartitionSpec as P


def local(tokens, expert_ids, route_levels, gate_proj, up_proj, down_proj):
    rows, width = tokens.shape
    experts = lax.axis_size("expert") // 2
    levels = jnp.sum(
        jnp.where(expert_ids[:, :, None] == jnp.arange(128, dtype=jnp.int32), route_levels[:, :, None], 0),
        axis=1,
    )
    carried = jnp.concatenate([tokens, levels.astype(jnp.bfloat16)], axis=1)
    everyone = lax.all_gather(carried, ("expert", "sub"), axis=0, tiled=True)
    x = everyone[:, :width]
    level = everyone[:, width:].astype(jnp.float32)
    mine = jnp.arange(128, dtype=jnp.int32) == lax.axis_index("expert") // 2
    share = jnp.sum(jnp.where(mine, level, 0.0), axis=1, keepdims=True) / jnp.sum(level, axis=1, keepdims=True)
    gate = jnp.dot(x, gate_proj[0], preferred_element_type=jnp.float32)
    up = jnp.dot(x, up_proj[0], preferred_element_type=jnp.float32)
    hidden = (jax.nn.silu(gate) * up * share).astype(jnp.bfloat16)
    part = jnp.dot(hidden, down_proj[0], preferred_element_type=jnp.float32).astype(jnp.bfloat16)
    return lax.psum_scatter(part, ("expert", "sub"), scatter_dimension=0, tiled=True)


def solution(mesh):
    return jax.shard_map(
        local,
        mesh=mesh,
        in_specs=(
            P(("replica", "expert", "sub"), None),
            P(("replica", "expert", "sub"), None),
            P(("replica", "expert", "sub"), None),
            P("expert", None, "sub"),
            P("expert", None, "sub"),
            P("expert", "sub", None),
        ),
        out_specs=P(("replica", "expert", "sub"), None),
        check_vma=False,
    )
```

```python
import functools
import math

import jax
import jax.numpy as jnp
from jax import lax
from jax.experimental import pallas as pl
from jax.experimental.pallas import tpu as pltpu
from jax.sharding import PartitionSpec as P

BF16, F32 = jnp.bfloat16, jnp.float32
LANES = 128
ORDER = (0, -1, 1, -2, 2, -3, 3, 4)
FORWARD, BACKWARD = 0, 1
HALF_RANKS = ((7, 6, 5, 4), (3, 2, 1, 0))
BLOCKS = ((0, 9), (9, 25), (25, 49), (49, 64))


def reach(place):
    return min(place % 8, -place % 8)


def slots():
    cells = [(y, x) for y in range(8) for x in range(8)]
    cells.sort(key=lambda c: max(reach(c[0]), reach(c[1])))
    return {cell: i for i, cell in enumerate(cells)}


SLOT = slots()


def slot(y, x):
    return SLOT[(y % 8, x % 8)]


def block_of(index):
    return next(b for b, (lo, hi) in enumerate(BLOCKS) if lo <= index < hi)


def kernel(
    tokens, levels, gate, up, down, out,
    x, w, wd, hs, hr, p, p0, r, s, rs, ss, osend, orecv,
    in_sem, w_sem, pair_send, pair_recv,
    g1_send, g1_recv, g2_send, g2_recv, d_send, d_recv, h_send, h_recv,
    b_send, b_recv, c_send, c_recv, o_send, o_recv,
):
    rows, width = tokens.shape
    half = width // 2
    part = half // 2
    chunk = 2 * rows
    side = math.isqrt(lax.axis_size("expert"))
    me = lax.axis_index("expert")
    core = lax.axis_index("sub")
    my_y, my_x = me // side, me % side
    quarter = hs.shape[1]
    other_at = half + LANES
    mine_from = pl.multiple_of(core * half, LANES)
    theirs_from = pl.multiple_of((1 - core) * half, LANES)
    sibling = {"sub": 1 - core}

    def neighbour(along_x, direction):
        step = 1 if direction == FORWARD else side - 1
        if along_x:
            return {"expert": my_y * side + (my_x + step) % side}
        return {"expert": ((my_y + step) % side) * side + my_x}

    lanes_of = (pl.ds(part, part + LANES), pl.ds(0, part))
    data_of = (pl.ds(part, part), pl.ds(0, part))
    there_of = (pl.ds(other_at + part, part), pl.ds(other_at, part))
    cut = ((pl.ds(part, 8 * LANES), pl.ds(part + 8 * LANES, 7 * LANES)), (pl.ds(0, part // 2), pl.ds(part // 2, part // 2)))

    def rows_of(index, count=1):
        return pl.ds(index * chunk, count * chunk)

    def remote(src, dst, send, recv, device):
        return pltpu.make_async_remote_copy(
            src_ref=src, dst_ref=dst, send_sem=send, recv_sem=recv, device_id=device,
            device_id_type=pl.DeviceIdType.MESH,
        )

    own_rows = pl.ds(pl.multiple_of(core * rows, rows), rows)
    loads = [
        pltpu.make_async_copy(tokens.at[:, pl.ds(mine_from, half)], x.at[own_rows, pl.ds(0, half)], in_sem.at[0]),
        pltpu.make_async_copy(levels, x.at[own_rows, pl.ds(half, LANES)], in_sem.at[1]),
        pltpu.make_async_copy(tokens.at[:, pl.ds(theirs_from, half)], x.at[own_rows, pl.ds(other_at, half)], in_sem.at[2]),
    ]
    weights = []
    for i, m in enumerate((gate, up)):
        for j, start in enumerate((mine_from, theirs_from)):
            weights.append(
                pltpu.make_async_copy(
                    m.at[0, pl.ds(start, half), :],
                    w.at[pl.ds(j * half, half), pl.ds(i * quarter, quarter)],
                    w_sem.at[2 * i + j],
                )
            )
    weights.append(pltpu.make_async_copy(down.at[0, :, pl.ds(mine_from, half)], wd.at[pl.ds(0, quarter), :], w_sem.at[4]))
    for c in loads + weights:
        c.start()

    barrier = pltpu.get_barrier_semaphore()
    for device in (
        sibling,
        neighbour(True, FORWARD),
        neighbour(True, BACKWARD),
        neighbour(False, FORWARD),
        neighbour(False, BACKWARD),
    ):
        pl.semaphore_signal(barrier, inc=1, device_id=device, device_id_type=pl.DeviceIdType.MESH)
    pl.semaphore_wait(barrier, 5)

    swaps = [
        remote(tokens.at[:, pl.ds(theirs_from, half)], x.at[own_rows, pl.ds(0, half)], pair_send.at[0], pair_recv.at[0], sibling),
        remote(levels, x.at[own_rows, pl.ds(half, LANES)], pair_send.at[1], pair_recv.at[1], sibling),
        remote(tokens.at[:, pl.ds(mine_from, half)], x.at[own_rows, pl.ds(other_at, half)], pair_send.at[2], pair_recv.at[2], sibling),
        remote(down.at[0, :, pl.ds(theirs_from, half)], wd.at[pl.ds(quarter, quarter), :], pair_send.at[3], pair_recv.at[3], sibling),
    ]
    for c in swaps:
        c.start()

    def cell(which, along, across):
        return slot(across, along) if which == 0 else slot(along, across)

    def line_copy(which, direction, k):
        sign = -1 if direction == FORWARD else 1
        lanes = lanes_of[which] if k < 4 else cut[which][direction]
        i = 4 * (2 * which + direction) + k - 1
        return remote(
            x.at[rows_of(cell(which, sign * (k - 1), 0)), lanes],
            x.at[rows_of(cell(which, sign * k, 0)), lanes],
            g1_send.at[i], g1_recv.at[i], neighbour(which == 0, direction),
        )

    def plane_copy(which, direction, k, rank):
        sign = -1 if direction == FORWARD else 1
        st = 2 * which + direction
        i = 28 * st + (8 * (k - 1) + rank if k < 4 else 24 + HALF_RANKS[direction].index(rank))
        return remote(
            x.at[rows_of(cell(which, ORDER[rank], sign * (k - 1))), lanes_of[which]],
            x.at[rows_of(cell(which, ORDER[rank], sign * k)), lanes_of[which]],
            g2_send.at[st], g2_recv.at[i], neighbour(which == 1, direction),
        )

    def hand_over(which, index):
        b = block_of(index)
        remote(
            x.at[rows_of(index), data_of[which]], x.at[rows_of(index), there_of[which]],
            d_send.at[b], d_recv.at[b], sibling,
        ).start()

    streams = [(which, direction) for which in (0, 1) for direction in (FORWARD, BACKWARD)]

    def line_arrives(k):
        for which, direction in streams:
            sign = -1 if direction == FORWARD else 1
            line_copy(which, direction, k).wait_recv()
            if k < 4:
                line_copy(which, direction, k + 1).start()
                rank = ORDER.index(sign * k)
                for d in (FORWARD, BACKWARD):
                    plane_copy(which, d, 1, rank).start()
                hand_over(which, cell(which, sign * k, 0))
        if k == 4:
            for which in (0, 1):
                for d in (FORWARD, BACKWARD):
                    plane_copy(which, d, 1, 7).start()
                hand_over(which, cell(which, 4, 0))

    def plane_arrives(k, rank):
        for which, direction in streams:
            sign = -1 if direction == FORWARD else 1
            if k == 4 and rank not in HALF_RANKS[direction]:
                continue
            plane_copy(which, direction, k, rank).wait_recv()
            if k < 3 or (k == 3 and rank in HALF_RANKS[direction]):
                plane_copy(which, direction, k + 1, rank).start()
            hand_over(which, cell(which, ORDER[rank], sign * k))

    def hidden_copy(b):
        lo, hi = BLOCKS[b]
        span = rows_of(lo, hi - lo)
        return remote(hs.at[span, :], hr.at[span, :], h_send.at[b], h_recv.at[b], sibling)

    def handed(b):
        lo, hi = BLOCKS[b]
        lo = max(lo, 1)
        span = rows_of(lo, hi - lo)
        return remote(x.at[span, pl.ds(0, half)], x.at[span, pl.ds(other_at, half)], d_send.at[b], d_recv.at[b], sibling)

    def compute(b):
        lo, hi = BLOCKS[b]
        handed(b).wait_recv()
        if b == 0:
            for c in weights[:4]:
                c.wait()
        span = rows_of(lo, hi - lo)
        pre = jnp.dot(x[span, pl.ds(0, half)], w[pl.ds(0, half), :], preferred_element_type=F32)
        pre += jnp.dot(x[span, pl.ds(other_at, half)], w[pl.ds(half, half), :], preferred_element_type=F32)
        level = x[span, pl.ds(half, LANES)].astype(F32)
        lane = lax.broadcasted_iota(jnp.int32, level.shape, 1)
        share = jnp.sum(jnp.where(lane == me // 2, level, 0.0), axis=1, keepdims=True)
        share = share / jnp.sum(level, axis=1, keepdims=True)
        g, u = pre[:, :quarter], pre[:, quarter:]
        hs[span, :] = (g / (1.0 + jnp.exp(-g)) * u * share).astype(BF16)
        hidden_copy(b).start()

    for c in loads:
        c.wait()
    for c in swaps[:2]:
        c.wait_recv()
    for which, direction in streams:
        line_copy(which, direction, 1).start()
    for which, direction in streams:
        plane_copy(which, direction, 1, 0).start()
    swaps[2].wait_recv()

    line_arrives(1)
    plane_arrives(1, 0)
    for k in (2, 3):
        line_arrives(k)
        plane_arrives(1, 2 * k - 3)
        plane_arrives(1, 2 * k - 2)
    line_arrives(4)
    for rank in (5, 6, 7):
        plane_arrives(1, rank)
    for k in (2, 3):
        for rank in range(8):
            plane_arrives(k, rank)
            if rank == 2:
                compute(k - 2)
    for i in range(4):
        for rank in (HALF_RANKS[1][3 - i], HALF_RANKS[0][3 - i]):
            plane_arrives(4, rank)
        if i == 0:
            compute(2)
    compute(3)

    def own_terms(which, across):
        index = [cell(which, ORDER[7 - j], across) for j in range(8)]
        a = jnp.concatenate([hs[rows_of(i), :] for i in index], axis=0)
        b = jnp.concatenate([hr[rows_of(i), :] for i in index], axis=0)
        lanes = data_of[which]
        return jnp.dot(a, wd[pl.ds(0, quarter), lanes], preferred_element_type=F32) + jnp.dot(
            b, wd[pl.ds(quarter, quarter), lanes], preferred_element_type=F32
        )

    def big_index(direction, k, rank):
        if k == 4:
            return HALF_RANKS[direction].index(rank)
        return 4 + 8 * (3 - k) + 7 - rank

    def big_copy(which, direction, k, rank):
        st = 2 * which + direction
        i = 28 * st + big_index(direction, k, rank)
        return remote(
            s.at[rows_of(i), :], r.at[rows_of(i), :], b_send.at[st], b_recv.at[i], neighbour(which == 1, direction)
        )

    def big_sends(k, rank):
        ready = []
        for which, direction in streams:
            if k == 4 and rank not in HALF_RANKS[direction]:
                continue
            st = 2 * which + direction
            plane = 2 * which if k == 4 else st
            value = p[pl.ds((plane * 8 + 7 - rank) * chunk, chunk), :]
            if k < 3 or (k == 3 and rank in HALF_RANKS[direction]):
                before = big_copy(which, direction, k + 1, rank)
                before.wait_recv()
                i = 28 * st + big_index(direction, k + 1, rank)
                value += r[rows_of(i), :].astype(F32)
            i = 28 * st + big_index(direction, k, rank)
            s[rows_of(i), :] = value.astype(BF16)
            ready.append(big_copy(which, direction, k, rank))
        for c in ready:
            c.start()

    def line_sum(which, rank):
        value = p0[pl.ds((which * 8 + 7 - rank) * chunk, chunk), :]
        for direction in (FORWARD, BACKWARD):
            big_copy(which, direction, 1, rank).wait_recv()
            i = 28 * (2 * which + direction) + big_index(direction, 1, rank)
            value += r[rows_of(i), :].astype(F32)
        return value

    def small_copy(which, direction, k):
        i = 4 * (2 * which + direction) + 4 - k
        lanes = pl.ds(0, part)
        if k == 4:
            lanes = pl.ds(direction * (part // 2), part // 2)
        return remote(
            ss.at[rows_of(i), lanes], rs.at[rows_of(i), lanes], c_send.at[i], c_recv.at[i],
            neighbour(which == 0, direction),
        )

    def small_sends(k):
        ready = []
        for which in (0, 1):
            whole = line_sum(which, 7) if k == 4 else None
            for direction in (FORWARD, BACKWARD):
                i = 4 * (2 * which + direction) + 4 - k
                if k == 4:
                    lanes = slice(direction * (part // 2), (direction + 1) * (part // 2))
                    ss[rows_of(i), lanes] = whole[:, lanes].astype(BF16)
                else:
                    value = line_sum(which, ORDER.index(k if direction == FORWARD else -k))
                    small_copy(which, direction, k + 1).wait_recv()
                    if k == 3:
                        lo = value[:, : part // 2]
                        hi = value[:, part // 2 :]
                        came = rs[rows_of(i - 1), pl.ds(direction * (part // 2), part // 2)].astype(F32)
                        if direction == FORWARD:
                            lo = lo + came
                        else:
                            hi = hi + came
                        ss[rows_of(i), pl.ds(0, part // 2)] = lo.astype(BF16)
                        ss[rows_of(i), pl.ds(part // 2, part // 2)] = hi.astype(BF16)
                    else:
                        ss[rows_of(i), :] = (value + rs[rows_of(i - 1), :].astype(F32)).astype(BF16)
                ready.append(small_copy(which, direction, k))
        for c in ready:
            c.start()

    def fill(k):
        if k == 4:
            for which in (0, 1):
                p[pl.ds(2 * which * 8 * chunk, 8 * chunk), :] = own_terms(which, 4)
            return
        for which, direction in streams:
            st = 2 * which + direction
            p[pl.ds(st * 8 * chunk, 8 * chunk), :] = own_terms(which, k if direction == FORWARD else -k)

    weights[4].wait()
    swaps[3].wait_recv()
    for b in range(len(BLOCKS)):
        hidden_copy(b).wait_recv()
    fill(4)
    for i in range(4):
        big_sends(4, HALF_RANKS[0][i])
        big_sends(4, HALF_RANKS[1][i])
    for k in (3, 2):
        fill(k)
        for rank in range(7, -1, -1):
            big_sends(k, rank)
    fill(1)
    for which in (0, 1):
        p0[pl.ds(which * 8 * chunk, 8 * chunk), :] = own_terms(which, 0)
    for rank in (7, 6, 5):
        big_sends(1, rank)
    small_sends(4)
    for rank in (4, 3):
        big_sends(1, rank)
    small_sends(3)
    for rank in (2, 1):
        big_sends(1, rank)
    small_sends(2)
    big_sends(1, 0)
    small_sends(1)

    own = [None, None]
    for which in (0, 1):
        value = line_sum(which, 0)
        for direction in (FORWARD, BACKWARD):
            small_copy(which, direction, 1).wait_recv()
            value += rs[rows_of(4 * (2 * which + direction) + 3), :].astype(F32)
        upper, lower = value[:rows], value[rows:]
        own[which] = jnp.where(core == 0, upper, lower).astype(BF16)
        osend[:, data_of[which]] = jnp.where(core == 0, lower, upper).astype(BF16)
    swap = remote(osend, orecv, o_send, o_recv, sibling)
    swap.start()
    for which in (0, 1):
        start = pl.multiple_of(core * half + (part if which == 0 else 0), LANES)
        out[:, pl.ds(start, part)] = own[which]
    swap.wait_recv()
    out[:, pl.ds(theirs_from, half)] = orecv[...]

    swap.wait_send()
    for c in swaps:
        c.wait_send()
    for which, direction in streams:
        st = 2 * which + direction
        for k in (1, 2, 3, 4):
            line_copy(which, direction, k).wait_send()
            small_copy(which, direction, k).wait_send()
        span = x.at[rows_of(0, 28), lanes_of[which]]
        remote(span, span, g2_send.at[st], g2_recv.at[28 * st], neighbour(which == 1, direction)).wait_send()
        span = s.at[rows_of(28 * st, 28), :]
        remote(span, span, b_send.at[st], b_recv.at[28 * st], neighbour(which == 1, direction)).wait_send()
    for b in range(len(BLOCKS)):
        handed(b).wait_send()
        hidden_copy(b).wait_send()


def local(tokens, expert_ids, route_levels, gate_proj, up_proj, down_proj):
    rows, width = tokens.shape
    quarter = gate_proj.shape[2]
    half, chunk = width // 2, 2 * rows
    part = half // 2
    chips = lax.axis_size("expert")
    levels = jnp.sum(
        jnp.where(expert_ids[:, :, None] == jnp.arange(LANES, dtype=jnp.int32), route_levels[:, :, None], 0), axis=1
    ).astype(BF16)
    dma = pltpu.SemaphoreType.DMA
    any_space = pl.BlockSpec(memory_space=pl.ANY)
    return pl.pallas_call(
        kernel,
        out_shape=jax.ShapeDtypeStruct((rows, width), BF16),
        in_specs=[any_space] * 5,
        out_specs=pl.BlockSpec(memory_space=pltpu.VMEM),
        scratch_shapes=[
            pltpu.VMEM((chips * chunk, width + LANES), BF16),
            pltpu.VMEM((width, 2 * quarter), BF16),
            pltpu.VMEM((2 * quarter, half), BF16),
            pltpu.VMEM((chips * chunk, quarter), BF16),
            pltpu.VMEM((chips * chunk, quarter), BF16),
            pltpu.VMEM((4 * 8 * chunk, part), F32),
            pltpu.VMEM((2 * 8 * chunk, part), F32),
            pltpu.VMEM((4 * 28 * chunk, part), BF16),
            pltpu.VMEM((4 * 28 * chunk, part), BF16),
            pltpu.VMEM((16 * chunk, part), BF16),
            pltpu.VMEM((16 * chunk, part), BF16),
            pltpu.VMEM((rows, half), BF16),
            pltpu.VMEM((rows, half), BF16),
            dma((3,)), dma((5,)), dma((4,)), dma((4,)),
            dma((16,)), dma((16,)), dma((4,)), dma((112,)), dma((4,)), dma((4,)), dma((4,)), dma((4,)),
            dma((4,)), dma((112,)), dma((16,)), dma((16,)), dma(()), dma(()),
        ],
        compiler_params=pltpu.CompilerParams(
            collective_id=0, has_side_effects=True, vmem_limit_bytes=66 * 1024 * 1000
        ),
    )(tokens, levels, gate_proj, up_proj, down_proj)


def solution(mesh):
    return jax.shard_map(
        local,
        mesh=mesh,
        in_specs=(
            P(("replica", "expert", "sub"), None),
            P(("replica", "expert", "sub"), None),
            P(("replica", "expert", "sub"), None),
            P("expert", None, "sub"),
            P("expert", None, "sub"),
            P("expert", "sub", None),
        ),
        out_specs=P(("replica", "expert", "sub"), None),
        check_vma=False,
    )
```
